32 devices in a mesh: ti: 4 (over z), tj: 8 (over y, x, core).
Axes of the slice: x: 2, y: 2, z: 4, core: 2. Of those that a mesh axis runs over, the one named last changes fastest.
Arguments:
- alignment_source: float32 [32, 128, 64], P('tj', 'ti'), may hold values from -6 to 6
- couple_source: float32 [128, 128, 128], P('ti', 'tj'), may hold values from -6 to 6
- tensor_operand_matrix: float32 [64, 64], replicated, may hold values from -0.75 to 0.75
- tensor_final_matrix: float32 [1024, 128], replicated, may hold values from -0.75 to 0.75
- mixing_content_matrix: float32 [64, 256], replicated, may hold values from -0.75 to 0.75
- mixing_switch_matrix: float32 [64, 256], replicated, may hold values from -0.75 to 0.75
- mixing_score_matrix: float32 [128, 8], replicated, may hold values from -48 to 48, as said below
- mixing_final_matrix: float32 [256, 64], replicated, may hold values from -0.375 to 0.375
- alignment_expand_matrix: float32 [64, 512], replicated, may hold values from -0.75 to 0.75
- alignment_shrink_matrix: float32 [256, 64], replicated, may hold values from -0.375 to 0.375
- couple_expand_matrix: float32 [128, 1024], replicated, may hold values from -0.5 to 0.5
- couple_shrink_matrix: float32 [512, 128], replicated, may hold values from -0.25 to 0.25
Outputs:
- alignment_result: float32 [32, 128, 64], P('tj', 'ti')
- couple_result: float32 [128, 128, 128], P('ti', 'tj')
The draws below stay inside these ranges and needn't reach their ends.
Inputs may be any that keep to these rules, and one draw needn't show every extreme that they name: `mixing_score_matrix`: each column is one head's logit projection.
All inputs are finite; a program needn't handle non-finite values.
Results may differ from the reference program's by a relative error of at most 0.00026.
Values sent between devices are 32-bit elements; how exact they have to be, the bound alone decides.
A program may use at most 64 MiB of HBM per device.

```python
import jax
import jax.numpy as jnp
from jax import lax

ALIGN_FEATURES = 64
C_Z = 128
FACTOR_WIDTH = 32
MEAN_GROUPS = 8
GROUP_FEATURES = 32
ALIGN_INNER_SIZE = 256
PAIR_HID = 512
RESIDUE_COUNT = 128
SEQUENCE_COUNT = 32


def draw_mixing_score_matrix(key, part):
    base = jnp.clip(jax.random.normal(key, (C_Z, MEAN_GROUPS), jnp.float32), -4.0, 4.0) * 0.3
    return base


def levels(own_key, dims, shards, least, top_value):
    factor_of, own = 1.0, jax.random.fold_in(own_key, 6)
    for axis_at, blocks in shards:
        steps = jnp.exp(jax.random.uniform(jax.random.fold_in(own, axis_at), (blocks,), jnp.float32, least / len(shards), top_value / len(shards)))
        factor_of = factor_of * jnp.repeat(steps, dims[axis_at] // blocks).reshape([-1 if axis == axis_at else 1 for axis in range(len(dims))])
    return factor_of


def noise(rng, extent, spread, most, shards=(), held_as=jnp.bfloat16):
    array = spread * jax.random.normal(rng, extent, jnp.float32)
    if shards:
        array = array * levels(rng, extent, shards, -0.22, 0.18)
    return jnp.clip(array, -most, most).astype(held_as)


def setup_inputs(seed: int = 0) -> dict:
    keys = jax.random.split(jax.random.key(seed), 13)
    alignment_source = noise(keys[0], (SEQUENCE_COUNT, RESIDUE_COUNT, ALIGN_FEATURES), 1.0, 6.0, ((0, 8), (1, 4)), jnp.float32)
    couple_source = noise(keys[1], (RESIDUE_COUNT, RESIDUE_COUNT, C_Z), 1.0, 6.0, ((0, 4), (1, 8)), jnp.float32)
    tensor_operand_matrix = noise(keys[2], (ALIGN_FEATURES, 2 * FACTOR_WIDTH), ALIGN_FEATURES ** -0.5, 0.75, (), jnp.float32)
    tensor_final_matrix = noise(keys[3], (FACTOR_WIDTH * FACTOR_WIDTH, C_Z), (FACTOR_WIDTH * FACTOR_WIDTH // 16) ** -0.5, 0.75, (), jnp.float32)
    mixing_content_matrix = noise(keys[4], (ALIGN_FEATURES, MEAN_GROUPS * GROUP_FEATURES), ALIGN_FEATURES ** -0.5, 0.75, (), jnp.float32)
    mixing_switch_matrix = noise(keys[5], (ALIGN_FEATURES, MEAN_GROUPS * GROUP_FEATURES), ALIGN_FEATURES ** -0.5, 0.75, (), jnp.float32)
    mixing_score_matrix = draw_mixing_score_matrix(jax.random.fold_in(keys[12], 71), 0)
    mixing_final_matrix = noise(keys[7], (MEAN_GROUPS * GROUP_FEATURES, ALIGN_FEATURES), (MEAN_GROUPS * GROUP_FEATURES) ** -0.5, 0.375, (), jnp.float32)
    alignment_expand_matrix = noise(keys[8], (ALIGN_FEATURES, 2 * ALIGN_INNER_SIZE), ALIGN_FEATURES ** -0.5, 0.75, (), jnp.float32)
    alignment_shrink_matrix = noise(keys[9], (ALIGN_INNER_SIZE, ALIGN_FEATURES), ALIGN_INNER_SIZE ** -0.5, 0.375, (), jnp.float32)
    couple_expand_matrix = noise(keys[10], (C_Z, 2 * PAIR_HID), C_Z ** -0.5, 0.5, (), jnp.float32)
    couple_shrink_matrix = noise(keys[11], (PAIR_HID, C_Z), PAIR_HID ** -0.5, 0.25, (), jnp.float32)
    return {"alignment_source": alignment_source, "couple_source": couple_source, "tensor_operand_matrix": tensor_operand_matrix, "tensor_final_matrix": tensor_final_matrix, "mixing_content_matrix": mixing_content_matrix, "mixing_switch_matrix": mixing_switch_matrix, "mixing_score_matrix": mixing_score_matrix, "mixing_final_matrix": mixing_final_matrix, "alignment_expand_matrix": alignment_expand_matrix, "alignment_shrink_matrix": alignment_shrink_matrix, "couple_expand_matrix": couple_expand_matrix, "couple_shrink_matrix": couple_shrink_matrix}


exact_arithmetic = lax.Precision.HIGHEST
epsilon = 1e-05

def feature_standardize(inputs):
    mean_val = lax.optimization_barrier(jnp.mean(inputs, axis=-1, keepdims=True))
    centred = inputs - mean_val
    variance = lax.optimization_barrier(jnp.mean(centred * centred, axis=-1, keepdims=True))
    return centred * lax.rsqrt(variance + epsilon)

def feedforward_block(inputs, gate_up, down):
    hidden = jnp.einsum('...c,cd->...d', inputs, gate_up, precision=exact_arithmetic)
    half_width = down.shape[0]
    activated = jax.nn.silu(hidden[..., :half_width]) * hidden[..., half_width:]
    return jnp.einsum('...c,cd->...d', activated, down, precision=exact_arithmetic)

def reference(alignment_source, couple_source, tensor_operand_matrix, tensor_final_matrix, mixing_content_matrix, mixing_switch_matrix, mixing_score_matrix, mixing_final_matrix, alignment_expand_matrix, alignment_shrink_matrix, couple_expand_matrix, couple_shrink_matrix):
    sequence_count_all = alignment_source.shape[0]
    residue_count_all = alignment_source.shape[1]
    alignment_standardized = feature_standardize(alignment_source)
    tensor_operands = jnp.einsum('zji,in->zjn', alignment_standardized, tensor_operand_matrix, precision=exact_arithmetic)
    left_proj = tensor_operands[..., :FACTOR_WIDTH]
    right_proj = tensor_operands[..., FACTOR_WIDTH:]
    block_size = min(32, residue_count_all)
    block_count = residue_count_all // block_size
    left_blocks = left_proj.reshape(sequence_count_all, block_count, block_size, FACTOR_WIDTH).transpose(1, 0, 2, 3)
    pair_blocks = couple_source.reshape(block_count, block_size, residue_count_all, C_Z)

    def pair_block(inputs_pair):
        left_block, pair_rows = inputs_pair
        outer_prod = jnp.einsum('sia,sjb->ijab', left_block, right_proj, precision=exact_arithmetic) / sequence_count_all
        flattened = outer_prod.reshape(-1, FACTOR_WIDTH * FACTOR_WIDTH)
        update = jnp.dot(flattened, tensor_final_matrix, precision=exact_arithmetic, preferred_element_type=jnp.float32)
        pair_mid = pair_rows + update.reshape(pair_rows.shape)
        pair_normed = feature_standardize(pair_mid)
        logits = jnp.einsum('ijc,ch->hij', pair_normed, mixing_score_matrix, precision=exact_arithmetic)
        pair_next = pair_mid + feedforward_block(pair_normed, couple_expand_matrix, couple_shrink_matrix)
        return (pair_next, logits)
    pair_next, logit_blocks = lax.map(pair_block, (left_blocks, pair_blocks))
    couple_result = pair_next.reshape(residue_count_all, residue_count_all, C_Z)
    logits = logit_blocks.transpose(1, 0, 2, 3).reshape(MEAN_GROUPS, residue_count_all, residue_count_all)
    row_max = lax.optimization_barrier(jnp.max(logits, axis=2, keepdims=True))
    exp_terms = jnp.exp(logits - row_max)
    weights = exp_terms / lax.optimization_barrier(jnp.sum(exp_terms, axis=2, keepdims=True))
    content_sequences = jnp.einsum('jzb,bq->jzq', alignment_standardized, mixing_content_matrix, precision=exact_arithmetic).reshape(sequence_count_all, residue_count_all, MEAN_GROUPS, GROUP_FEATURES)
    sigmoid_switch = jax.nn.sigmoid(jnp.einsum('zji,in->zjn', alignment_standardized, mixing_switch_matrix, precision=exact_arithmetic))
    group_mixed = jnp.einsum('hij,sjhc->sihc', weights, content_sequences, precision=exact_arithmetic).reshape(sequence_count_all, residue_count_all, MEAN_GROUPS * GROUP_FEATURES)
    alignment_between = alignment_source + jnp.einsum('xvr,rq->xvq', sigmoid_switch * group_mixed, mixing_final_matrix, precision=exact_arithmetic)
    alignment_result = alignment_between + feedforward_block(feature_standardize(alignment_between), alignment_expand_matrix, alignment_shrink_matrix)
    return (alignment_result, couple_result)
```

```python
import functools

import jax
import jax.numpy as jnp
from jax import lax
from jax.experimental import pallas as pl
from jax.experimental.pallas import tpu as pltpu
from jax.sharding import PartitionSpec as P

F32, BF16 = jnp.float32, jnp.bfloat16
HI = lax.Precision.HIGHEST
MESH = pl.DeviceIdType.MESH
LANES = 128
EPS = 1e-05


def ln(x):
    c = x - jnp.mean(x, axis=-1, keepdims=True)
    return c * lax.rsqrt(jnp.mean(c * c, axis=-1, keepdims=True) + EPS)


def split2(x):
    hi = x.astype(BF16)
    return hi, (x - hi.astype(F32)).astype(BF16)


def split3(x):
    hi = x.astype(BF16)
    r = x - hi.astype(F32)
    mid = r.astype(BF16)
    return hi, mid, (r - mid.astype(F32)).astype(BF16)


def bdot(x, w):
    return jnp.dot(x, w, preferred_element_type=F32)


def dot3(x, w):
    xh, xl = split2(x)
    wh, wl = w
    if x.shape[1] % LANES == 0:
        return bdot(
            jnp.concatenate([xh, xl, xh], axis=1), jnp.concatenate([wh, wh, wl], axis=0)
        )
    return bdot(xh, wh) + (bdot(xl, wh) + bdot(xh, wl))


def lane_iota(rows):
    return lax.broadcasted_iota(jnp.int32, (rows, LANES), 1)


def block_transpose(arrs):
    n = len(arrs)
    width = LANES // n
    lane = lane_iota(arrs[0].shape[0])
    arrs = list(arrs)
    bit = n // 2
    while bit:
        step = bit * width
        low = (lane // step) % 2 == 0
        for t in range(n):
            if t & bit == 0:
                x, y = arrs[t], arrs[t + bit]
                arrs[t] = jnp.where(low, x, pltpu.roll(y, step, 1))
                arrs[t + bit] = jnp.where(low, pltpu.roll(x, LANES - step, 1), y)
        bit //= 2
    return arrs


def kernel(nt, nj, dims, *refs):
    rows, toks, cols, ch, cz, width, heads, feat = dims
    hbm = refs[:12]
    out_msa, out_pair = refs[12:14]
    vm = refs[14:26]
    (
        left_own, right_own, norm_own, logit_own,
        left_all, right_all, norm_all, logit_all,
        outer_flat, pair_mid_ref, pair_norm_ref, pair_out, msa_out,
        in_sem, out_sem, left_send, right_send, norm_send, logit_send,
        left_recv, right_recv, norm_recv, logit_recv,
    ) = refs[26:]
    ti, tj = lax.axis_index("ti"), lax.axis_index("tj")
    ratio = toks // cols
    seqs = rows * nj

    order = (0, 2, 1, 3, 4, 5, 6, 7, 8, 9, 10, 11)
    loads = {k: pltpu.make_async_copy(hbm[k], vm[k], in_sem.at[k]) for k in range(12)}
    for k in order:
        loads[k].start()

    barrier = pltpu.get_barrier_semaphore()
    for d in range(1, nj):
        pl.semaphore_signal(barrier, inc=1, device_id=(ti, (tj + d) % nj), device_id_type=MESH)
    for d in range(1, nt):
        pl.semaphore_signal(barrier, inc=1, device_id=((ti + d) % nt, tj), device_id_type=MESH)
    source_ti = tj // ratio
    is_holder = source_ti == ti
    for d in range(nj):
        if d == 0:
            @pl.when(jnp.logical_not(is_holder))
            def _():
                pl.semaphore_signal(
                    barrier, inc=1, device_id=(source_ti, tj), device_id_type=MESH
                )
        else:
            pl.semaphore_signal(
                barrier, inc=1, device_id=(source_ti, (tj + d) % nj), device_id_type=MESH
            )

    loads[0].wait()
    loads[2].wait()
    src = vm[0][...]
    norm = ln(src)
    operand = vm[2][...]
    rep = (
        lax.broadcasted_iota(jnp.int32, (2 * width, LANES), 0)
        == width + lax.broadcasted_iota(jnp.int32, (2 * width, LANES), 1) % width
    ).astype(F32)
    right_w = jnp.dot(operand, rep, precision=HI, preferred_element_type=F32)
    right = jnp.dot(norm, right_w, precision=HI, preferred_element_type=F32)
    groups = LANES // width
    sub8 = lax.broadcasted_iota(jnp.int32, (8, LANES), 0)
    lane8 = lax.broadcasted_iota(jnp.int32, (8, LANES), 1) // width
    for half in range(ratio):
        for s2 in range(0, rows, 2):
            parts = []
            for s in (s2, s2 + 1):
                at = s * toks + half * cols
                acc = jnp.where(
                    lane8 == sub8 // 4, right[at : at + 8],
                    jnp.where(lane8 == 2 + sub8 // 4, right[at + 8 : at + 16], 0.0),
                )
                parts.append(acc + pltpu.roll(acc, 4, 0))
            right_own[half, s2 * 4 : s2 * 4 + 8, :] = jnp.where(sub8 < 4, parts[0], parts[1])
    norm_rep = jnp.concatenate(
        [norm[s * toks : (s + 1) * toks] for s in range(rows) for _ in range(groups)], axis=0
    )
    left = lax.dot_general(
        operand.T[:width], norm_rep, (((1,), (1,)), ((), ())),
        precision=HI, preferred_element_type=F32,
    )
    for s in range(rows):
        acc = left[0:8, s * LANES : (s + 1) * LANES]
        for q in range(1, groups):
            acc = jnp.where(
                lane8 == q, left[q * 8 : q * 8 + 8, s * LANES : (s + 1) * LANES], acc
            )
        left_own[s * 8 : s * 8 + 8, :] = acc
    packed = rows * toks // 2
    norm_own[...] = jnp.concatenate([norm[:packed], norm[packed:]], axis=1)

    greet = (nj - 1) + (nt - 1) + nt * ratio
    @pl.when(is_holder)
    def _():
        pl.semaphore_wait(barrier, greet - 1)

    @pl.when(jnp.logical_not(is_holder))
    def _():
        pl.semaphore_wait(barrier, greet)

    def remote(src_ref, dst_ref, send, recv, device):
        return pltpu.make_async_remote_copy(
            src_ref=src_ref, dst_ref=dst_ref, send_sem=send, recv_sem=recv,
            device_id=device, device_id_type=MESH,
        )

    sends = []
    right_to = []
    for d in range(nt):
        for c in range(ratio):
            k = d * ratio + c
            to = ((ti + d) % nt, ti * ratio + c)
            copy = remote(
                right_own.at[c], right_all.at[tj], right_send.at[k], right_recv.at[tj], to
            )
            if d == 0:
                mine = ti * ratio + c == tj
                right_to.append((copy, mine))

                @pl.when(mine)
                def _():
                    pltpu.make_async_copy(
                        right_own.at[c], right_all.at[tj], right_recv.at[tj]
                    ).start()

                @pl.when(jnp.logical_not(mine))
                def _():
                    copy.start()
            else:
                copy.start()
                sends.append(copy)
    pltpu.make_async_copy(left_own, left_all.at[tj], left_recv.at[tj]).start()
    for d in range(1, nj):
        copy = remote(
            left_own, left_all.at[tj], left_send.at[d], left_recv.at[tj], (ti, (tj + d) % nj)
        )
        copy.start()
        sends.append(copy)
    pltpu.make_async_copy(norm_own, norm_all.at[ti], norm_recv.at[ti]).start()
    for d in range(1, nt):
        copy = remote(
            norm_own, norm_all.at[ti], norm_send.at[d], norm_recv.at[ti], ((ti + d) % nt, tj)
        )
        copy.start()
        sends.append(copy)

    for k in (5, 6, 3, 1):
        loads[k].wait()
    gates_in = dot3(norm, split2(vm[5][...]))
    gates = 1.0 / (1.0 + jnp.exp(-gates_in))
    spread = (
        lax.broadcasted_iota(jnp.int32, (heads, LANES), 0)
        == lax.broadcasted_iota(jnp.int32, (heads, LANES), 1) // (LANES // heads)
    ).astype(F32)
    score = jnp.dot(vm[6][...], spread, precision=HI, preferred_element_type=F32)
    final = vm[3][...]
    final_perm = jnp.concatenate(
        [
            final[(q * 8 + g) * width : (q * 8 + g + 1) * width]
            for g in range(width // groups) for q in range(groups)
        ],
        axis=0,
    )

    for p in range(nj):
        pltpu.make_async_copy(left_own, left_all.at[p], left_recv.at[p]).wait()
        pltpu.make_async_copy(right_own.at[0], right_all.at[p], right_recv.at[p]).wait()

    tiles = cols // 4
    left_2d = left_all.reshape(seqs * 8, LANES)
    right_2d = right_all.reshape(seqs * 4, LANES)
    r_cat = jnp.concatenate(
        [right_2d[pl.ds(t, seqs, stride=4), :] for t in range(tiles)], axis=1
    )
    rh, rm, rl = split3(r_cat)
    r_stack = jnp.concatenate([rh, rm, rh, rm, rl, rh], axis=0)
    for g in range(width // groups):
        lh, lm, ll = split3(left_2d[pl.ds(g, seqs, stride=8), :])
        l_stack = jnp.concatenate([lh, lh, lm, lm, lh, ll], axis=0)
        outer = lax.dot_general(
            l_stack, r_stack, (((0,), (0,)), ((), ())), preferred_element_type=F32
        )
        for t in range(tiles):
            blocks = block_transpose(
                [outer[q * toks : (q + 1) * toks, t * LANES : (t + 1) * LANES] for q in range(groups)]
            )
            for q in range(groups):
                at = (t * groups + q) * toks
                outer_flat[at : at + toks, g * LANES : (g + 1) * LANES] = blocks[q]
    update = jnp.dot(
        outer_flat[...], final_perm, precision=HI, preferred_element_type=F32
    ) * (1.0 / seqs)
    token_of = [q * 4 + t for t in range(tiles) for q in range(groups)]
    pair_in = jnp.concatenate([vm[1][pl.ds(j, toks, stride=cols), :] for j in token_of], axis=0)
    pair_mid = pair_in + update
    pair_mid_ref[...] = pair_mid
    pair_norm = ln(pair_mid)
    pair_norm_ref[...] = pair_norm
    logits = jnp.dot(pair_norm, score, precision=HI, preferred_element_type=F32)
    slot = lane_iota(toks) % cols
    acc = logits[:toks]
    for p in range(1, cols):
        acc = jnp.where(slot == token_of[p], logits[p * toks : (p + 1) * toks], acc)
    logit_own[...] = acc
    pltpu.make_async_copy(logit_own, logit_all.at[tj], logit_recv.at[tj]).start()
    for d in range(1, nj):
        copy = remote(
            logit_own, logit_all.at[tj], logit_send.at[d], logit_recv.at[tj], (ti, (tj + d) % nj)
        )
        copy.start()
        sends.append(copy)

    loads[10].wait()
    loads[11].wait()
    expand = split2(vm[10][...])
    shrink = split2(vm[11][...])
    hid = vm[11].shape[0]
    chunk = cols * toks // 4
    for b in range(4):
        x = pair_norm_ref[b * chunk : (b + 1) * chunk]
        hidden = dot3(x, expand)
        gate = hidden[:, :hid]
        act = gate / (1.0 + jnp.exp(-gate)) * hidden[:, hid:]
        res = pair_mid_ref[b * chunk : (b + 1) * chunk] + dot3(act, shrink)
        for p in range(chunk // toks):
            j = token_of[b * (chunk // toks) + p]
            pair_out[pl.ds(j, toks, stride=cols), :] = res[p * toks : (p + 1) * toks]
    pair_store = pltpu.make_async_copy(pair_out, out_pair, out_sem.at[0])
    pair_store.start()

    loads[4].wait()
    for p in range(nt):
        pltpu.make_async_copy(norm_own, norm_all.at[p], norm_recv.at[p]).wait()
    content = vm[4][...]
    zero = jnp.zeros_like(content)
    content2 = jnp.concatenate(
        [jnp.concatenate([content, zero], axis=1), jnp.concatenate([zero, content], axis=1)], axis=0
    )
    values = dot3(norm_all.reshape(nt * packed, LANES)[...], split2(content2))
    hf = heads * feat
    per = rows // 2
    values = jnp.concatenate(
        [
            jnp.concatenate(
                [
                    values[t * packed + lo * toks : t * packed + (lo + 1) * toks, up * hf : (up + 1) * hf]
                    for t in range(nt)
                ],
                axis=0,
            )
            for up in range(2) for lo in range(per)
        ],
        axis=1,
    )
    values = split2(values)
    for k in (7, 8, 9):
        loads[k].wait()
    mix_final = split2(vm[7][...])
    msa_expand = split2(vm[8][...])
    msa_shrink = split2(vm[9][...])

    for p in range(nj):
        pltpu.make_async_copy(logit_own, logit_all.at[p], logit_recv.at[p]).wait()
    scores = jnp.concatenate(
        [
            jnp.concatenate(block_transpose([logit_all[g + p] for p in range(heads)]), axis=0)
            for g in range(0, nj, heads)
        ],
        axis=1,
    )
    exps = jnp.exp(scores - jnp.max(scores, axis=-1, keepdims=True))
    weights = exps / jnp.sum(exps, axis=-1, keepdims=True)
    mixed = dot3(weights, values)
    head_of = lax.broadcasted_iota(jnp.int32, (toks, hf), 1) // feat
    averaged = []
    for s in range(rows):
        acc = mixed[:toks, s * hf : (s + 1) * hf]
        for h in range(1, heads):
            acc = jnp.where(
                head_of == h, mixed[h * toks : (h + 1) * toks, s * hf : (s + 1) * hf], acc
            )
        averaged.append(acc)
    averaged = jnp.concatenate(averaged, axis=0)
    msa_mid = src + dot3(gates * averaged, mix_final)
    hidden = dot3(ln(msa_mid), msa_expand)
    inner = vm[9].shape[0]
    gate = hidden[:, :inner]
    act = gate / (1.0 + jnp.exp(-gate)) * hidden[:, inner:]
    msa_out[...] = msa_mid + dot3(act, msa_shrink)
    msa_store = pltpu.make_async_copy(msa_out, out_msa, out_sem.at[1])
    msa_store.start()

    for copy in sends:
        copy.wait_send()
    for copy, mine in right_to:
        @pl.when(jnp.logical_not(mine))
        def _():
            copy.wait_send()
    pair_store.wait()
    msa_store.wait()


def shards(nt, nj, *args):
    rows, toks, ch = args[0].shape
    cols, cz = args[1].shape[1:]
    width = args[2].shape[1] // 2
    heads = args[6].shape[1]
    feat = args[4].shape[1] // heads
    dims = (rows, toks, cols, ch, cz, width, heads, feat)
    flat = (args[0].reshape(rows * toks, ch), args[1].reshape(toks * cols, cz)) + args[2:]
    pairs = toks * cols
    packed = rows * toks // 2
    dma = pltpu.SemaphoreType.DMA
    v = lambda *shape: pltpu.VMEM(shape, F32)
    outs = pl.pallas_call(
        functools.partial(kernel, nt, nj, dims),
        out_shape=(
            jax.ShapeDtypeStruct((rows * toks, ch), F32),
            jax.ShapeDtypeStruct((pairs, cz), F32),
        ),
        in_specs=[pl.BlockSpec(memory_space=pl.ANY)] * 12,
        out_specs=(pl.BlockSpec(memory_space=pl.ANY),) * 2,
        scratch_shapes=[v(*a.shape) for a in flat]
        + [
            v(rows * 8, LANES), v(toks // cols, rows * 4, LANES), v(packed, LANES), v(toks, LANES),
            v(nj, rows * 8, LANES), v(nj, rows * 4, LANES), v(nt, packed, LANES), v(nj, toks, LANES),
            v(pairs, width * width), v(pairs, cz), v(pairs, cz), v(pairs, cz), v(rows * toks, ch),
            dma((12,)), dma((2,)), dma((nj,)), dma((nt * toks // cols,)), dma((nt,)), dma((nj,)),
            dma((nj,)), dma((nj,)), dma((nt,)), dma((nj,)),
        ],
        compiler_params=pltpu.CompilerParams(
            collective_id=0, has_side_effects=True, vmem_limit_bytes=48 * 1024 * 1024
        ),
    )(*flat)
    return outs[0].reshape(args[0].shape), outs[1].reshape(args[1].shape)


def solution(mesh):
    in_specs = (P("tj", "ti", None), P("ti", "tj", None)) + (P(),) * 10
    out_specs = (P("tj", "ti", None), P("ti", "tj", None))
    return jax.shard_map(
        functools.partial(shards, mesh.shape["ti"], mesh.shape["tj"]),
        mesh=mesh, in_specs=in_specs, out_specs=out_specs, check_vma=False,
    )
```

```python
import functools

import jax
import jax.numpy as jnp
from jax import lax
from jax.experimental import pallas as pl
from jax.experimental.pallas import tpu as pltpu
from jax.sharding import PartitionSpec as P

F32, BF16 = jnp.float32, jnp.bfloat16
HI = lax.Precision.HIGHEST
MESH = pl.DeviceIdType.MESH
LANES = 128
EPS = 1e-05


def ln(x):
    c = x - jnp.mean(x, axis=-1, keepdims=True)
    return c * lax.rsqrt(jnp.mean(c * c, axis=-1, keepdims=True) + EPS)


def split2(x):
    hi = x.astype(BF16)
    return hi, (x - hi.astype(F32)).astype(BF16)


def split3(x):
    hi = x.astype(BF16)
    r = x - hi.astype(F32)
    mid = r.astype(BF16)
    return hi, mid, (r - mid.astype(F32)).astype(BF16)


def bdot(x, w):
    return jnp.dot(x, w, preferred_element_type=F32)


def dot3(x, w):
    xh, xl = split2(x)
    wh, wl = w
    if x.shape[1] % LANES == 0:
        return bdot(
            jnp.concatenate([xh, xl, xh], axis=1), jnp.concatenate([wh, wh, wl], axis=0)
        )
    return bdot(xh, wh) + (bdot(xl, wh) + bdot(xh, wl))


def lane_iota(rows):
    return lax.broadcasted_iota(jnp.int32, (rows, LANES), 1)


def block_transpose(arrs):
    n = len(arrs)
    width = LANES // n
    lane = lane_iota(arrs[0].shape[0])
    arrs = list(arrs)
    bit = n // 2
    while bit:
        step = bit * width
        low = (lane // step) % 2 == 0
        for t in range(n):
            if t & bit == 0:
                x, y = arrs[t], arrs[t + bit]
                arrs[t] = jnp.where(low, x, pltpu.roll(y, step, 1))
                arrs[t + bit] = jnp.where(low, pltpu.roll(x, LANES - step, 1), y)
        bit //= 2
    return arrs


def kernel(nt, nj, dims, *refs):
    rows, toks, cols, ch, cz, width, heads, feat = dims
    hbm = refs[:12]
    out_msa, out_pair = refs[12:14]
    vm = refs[14:26]
    (
        left_own, right_own, norm_own, logit_own,
        left_all, right_all, norm_all, logit_all,
        outer_flat, pair_mid_ref, pair_norm_ref, pair_out, msa_out,
        in_sem, out_sem, left_send, right_send, norm_send, logit_send,
        left_recv, right_recv, norm_recv, logit_recv,
    ) = refs[26:]
    ti, tj = lax.axis_index("ti"), lax.axis_index("tj")
    ratio = toks // cols
    seqs = rows * nj

    order = (0, 2, 1, 3, 4, 5, 6, 7, 8, 9, 10, 11)
    loads = {k: pltpu.make_async_copy(hbm[k], vm[k], in_sem.at[k]) for k in range(12)}
    for k in order:
        loads[k].start()

    barrier = pltpu.get_barrier_semaphore()
    for d in range(1, nj):
        pl.semaphore_signal(barrier, inc=1, device_id=(ti, (tj + d) % nj), device_id_type=MESH)
    for d in range(1, nt):
        pl.semaphore_signal(barrier, inc=1, device_id=((ti + d) % nt, tj), device_id_type=MESH)
    source_ti = tj // ratio
    is_holder = source_ti == ti
    for d in range(nj):
        if d == 0:
            @pl.when(jnp.logical_not(is_holder))
            def _():
                pl.semaphore_signal(
                    barrier, inc=1, device_id=(source_ti, tj), device_id_type=MESH
                )
        else:
            pl.semaphore_signal(
                barrier, inc=1, device_id=(source_ti, (tj + d) % nj), device_id_type=MESH
            )

    loads[0].wait()
    loads[2].wait()
    src = vm[0][...]
    norm = ln(src)
    operand = vm[2][...]
    rep = (
        lax.broadcasted_iota(jnp.int32, (2 * width, LANES), 0)
        == width + lax.broadcasted_iota(jnp.int32, (2 * width, LANES), 1) % width
    ).astype(F32)
    right_w = jnp.dot(operand, rep, precision=HI, preferred_element_type=F32)
    right = jnp.dot(norm, right_w, precision=HI, preferred_element_type=F32)
    groups = LANES // width
    sub8 = lax.broadcasted_iota(jnp.int32, (8, LANES), 0)
    lane8 = lax.broadcasted_iota(jnp.int32, (8, LANES), 1) // width
    for half in range(ratio):
        for s2 in range(0, rows, 2):
            parts = []
            for s in (s2, s2 + 1):
                at = s * toks + half * cols
                acc = jnp.where(
                    lane8 == sub8 // 4, right[at : at + 8],
                    jnp.where(lane8 == 2 + sub8 // 4, right[at + 8 : at + 16], 0.0),
                )
                parts.append(acc + pltpu.roll(acc, 4, 0))
            right_own[half, s2 * 4 : s2 * 4 + 8, :] = jnp.where(sub8 < 4, parts[0], parts[1])
    norm_rep = jnp.concatenate(
        [norm[s * toks : (s + 1) * toks] for s in range(rows) for _ in range(groups)], axis=0
    )
    left = lax.dot_general(
        operand.T[:width], norm_rep, (((1,), (1,)), ((), ())),
        precision=HI, preferred_element_type=F32,
    )
    for s in range(rows):
        acc = left[0:8, s * LANES : (s + 1) * LANES]
        for q in range(1, groups):
            acc = jnp.where(
                lane8 == q, left[q * 8 : q * 8 + 8, s * LANES : (s + 1) * LANES], acc
            )
        left_own[s * 8 : s * 8 + 8, :] = acc
    packed = rows * toks // 2
    norm_own[...] = jnp.concatenate([norm[:packed], norm[packed:]], axis=1)

    greet = (nj - 1) + (nt - 1) + nt * ratio
    @pl.when(is_holder)
    def _():
        pl.semaphore_wait(barrier, greet - 1)

    @pl.when(jnp.logical_not(is_holder))
    def _():
        pl.semaphore_wait(barrier, greet)

    def remote(src_ref, dst_ref, send, recv, device):
        return pltpu.make_async_remote_copy(
            src_ref=src_ref, dst_ref=dst_ref, send_sem=send, recv_sem=recv,
            device_id=device, device_id_type=MESH,
        )

    sends = []
    right_to = []
    for d in range(nt):
        for c in range(ratio):
            k = d * ratio + c
            to = ((ti + d) % nt, ti * ratio + c)
            copy = remote(
                right_own.at[c], right_all.at[tj], right_send.at[k], right_recv.at[tj], to
            )
            if d == 0:
                mine = ti * ratio + c == tj
                right_to.append((copy, mine))

                @pl.when(mine)
                def _():
                    pltpu.make_async_copy(
                        right_own.at[c], right_all.at[tj], right_recv.at[tj]
                    ).start()

                @pl.when(jnp.logical_not(mine))
                def _():
                    copy.start()
            else:
                copy.start()
                sends.append(copy)
    pltpu.make_async_copy(left_own, left_all.at[tj], left_recv.at[tj]).start()
    for d in range(1, nj):
        copy = remote(
            left_own, left_all.at[tj], left_send.at[d], left_recv.at[tj], (ti, (tj + d) % nj)
        )
        copy.start()
        sends.append(copy)
    pltpu.make_async_copy(norm_own, norm_all.at[ti], norm_recv.at[ti]).start()
    for d in range(1, nt):
        copy = remote(
            norm_own, norm_all.at[ti], norm_send.at[d], norm_recv.at[ti], ((ti + d) % nt, tj)
        )
        copy.start()
        sends.append(copy)

    for k in (5, 6, 3, 1):
        loads[k].wait()
    gates_in = dot3(norm, split2(vm[5][...]))
    gates = 1.0 / (1.0 + jnp.exp(-gates_in))
    spread = (
        lax.broadcasted_iota(jnp.int32, (heads, LANES), 0)
        == lax.broadcasted_iota(jnp.int32, (heads, LANES), 1) // (LANES // heads)
    ).astype(F32)
    score = jnp.dot(vm[6][...].T, spread, precision=HI, preferred_element_type=F32)
    final = vm[3][...]
    final_perm = jnp.concatenate(
        [
            final[(q * 8 + g) * width : (q * 8 + g + 1) * width]
            for g in range(width // groups) for q in range(groups)
        ],
        axis=0,
    )

    for p in range(nj):
        pltpu.make_async_copy(left_own, left_all.at[p], left_recv.at[p]).wait()
        pltpu.make_async_copy(right_own.at[0], right_all.at[p], right_recv.at[p]).wait()

    tiles = cols // 4
    left_2d = left_all.reshape(seqs * 8, LANES)
    right_2d = right_all.reshape(seqs * 4, LANES)
    r_cat = jnp.concatenate(
        [right_2d[pl.ds(t, seqs, stride=4), :] for t in range(tiles)], axis=1
    )
    rh, rm, rl = split3(r_cat)
    r_stack = jnp.concatenate([rh, rm, rh, rm, rl, rh], axis=0)
    for g in range(width // groups):
        lh, lm, ll = split3(left_2d[pl.ds(g, seqs, stride=8), :])
        l_stack = jnp.concatenate([lh, lh, lm, lm, lh, ll], axis=0)
        outer = lax.dot_general(
            l_stack, r_stack, (((0,), (0,)), ((), ())), preferred_element_type=F32
        )
        for t in range(tiles):
            blocks = block_transpose(
                [outer[q * toks : (q + 1) * toks, t * LANES : (t + 1) * LANES] for q in range(groups)]
            )
            for q in range(groups):
                at = (t * groups + q) * toks
                outer_flat[at : at + toks, g * LANES : (g + 1) * LANES] = blocks[q]
    update = jnp.dot(
        outer_flat[...], final_perm, precision=HI, preferred_element_type=F32
    ) * (1.0 / seqs)
    token_of = [q * 4 + t for t in range(tiles) for q in range(groups)]
    pair_in = jnp.concatenate([vm[1][pl.ds(j, toks, stride=cols), :] for j in token_of], axis=0)
    pair_mid = pair_in + update
    pair_mid_ref[...] = pair_mid
    pair_norm = ln(pair_mid)
    pair_norm_ref[...] = pair_norm
    logits = jnp.dot(pair_norm, score, precision=HI, preferred_element_type=F32)
    slot = lane_iota(toks) % cols
    acc = logits[:toks]
    for p in range(1, cols):
        acc = jnp.where(slot == token_of[p], logits[p * toks : (p + 1) * toks], acc)
    logit_own[...] = acc
    pltpu.make_async_copy(logit_own, logit_all.at[tj], logit_recv.at[tj]).start()
    for d in range(1, nj):
        copy = remote(
            logit_own, logit_all.at[tj], logit_send.at[d], logit_recv.at[tj], (ti, (tj + d) % nj)
        )
        copy.start()
        sends.append(copy)

    loads[10].wait()
    loads[11].wait()
    expand = split2(vm[10][...])
    shrink = split2(vm[11][...])
    hid = vm[11].shape[0]
    chunk = cols * toks // 4
    for b in range(4):
        x = pair_norm_ref[b * chunk : (b + 1) * chunk]
        hidden = dot3(x, expand)
        gate = hidden[:, :hid]
        act = gate / (1.0 + jnp.exp(-gate)) * hidden[:, hid:]
        res = pair_mid_ref[b * chunk : (b + 1) * chunk] + dot3(act, shrink)
        for p in range(chunk // toks):
            j = token_of[b * (chunk // toks) + p]
            pair_out[pl.ds(j, toks, stride=cols), :] = res[p * toks : (p + 1) * toks]
    pair_store = pltpu.make_async_copy(pair_out, out_pair, out_sem.at[0])
    pair_store.start()

    loads[4].wait()
    for p in range(nt):
        pltpu.make_async_copy(norm_own, norm_all.at[p], norm_recv.at[p]).wait()
    content = vm[4][...]
    zero = jnp.zeros_like(content)
    content2 = jnp.concatenate(
        [jnp.concatenate([content, zero], axis=1), jnp.concatenate([zero, content], axis=1)], axis=0
    )
    values = dot3(norm_all.reshape(nt * packed, LANES)[...], split2(content2))
    hf = heads * feat
    per = rows // 2
    values = jnp.concatenate(
        [
            jnp.concatenate(
                [
                    values[t * packed + lo * toks : t * packed + (lo + 1) * toks, up * hf : (up + 1) * hf]
                    for t in range(nt)
                ],
                axis=0,
            )
            for up in range(2) for lo in range(per)
        ],
        axis=1,
    )
    values = split2(values)
    for k in (7, 8, 9):
        loads[k].wait()
    mix_final = split2(vm[7][...].T)
    msa_expand = split2(vm[8][...])
    msa_shrink = split2(vm[9][...].T)

    for p in range(nj):
        pltpu.make_async_copy(logit_own, logit_all.at[p], logit_recv.at[p]).wait()
    scores = jnp.concatenate(
        [
            jnp.concatenate(block_transpose([logit_all[g + p] for p in range(heads)]), axis=0)
            for g in range(0, nj, heads)
        ],
        axis=1,
    )
    exps = jnp.exp(scores - jnp.max(scores, axis=-1, keepdims=True))
    weights = exps / jnp.sum(exps, axis=-1, keepdims=True)
    mixed = dot3(weights, values)
    head_of = lax.broadcasted_iota(jnp.int32, (toks, hf), 1) // feat
    averaged = []
    for s in range(rows):
        acc = mixed[:toks, s * hf : (s + 1) * hf]
        for h in range(1, heads):
            acc = jnp.where(
                head_of == h, mixed[h * toks : (h + 1) * toks, s * hf : (s + 1) * hf], acc
            )
        averaged.append(acc)
    averaged = jnp.concatenate(averaged, axis=0)
    msa_mid = src + dot3(gates * averaged, mix_final)
    hidden = dot3(ln(msa_mid), msa_expand)
    inner = vm[9].shape[1]
    gate = hidden[:, :inner]
    act = gate / (1.0 + jnp.exp(-gate)) * hidden[:, inner:]
    msa_out[...] = msa_mid + dot3(act, msa_shrink)
    msa_store = pltpu.make_async_copy(msa_out, out_msa, out_sem.at[1])
    msa_store.start()

    for copy in sends:
        copy.wait_send()
    for copy, mine in right_to:
        @pl.when(jnp.logical_not(mine))
        def _():
            copy.wait_send()
    pair_store.wait()
    msa_store.wait()


def shards(nt, nj, *args):
    rows, toks, ch = args[0].shape
    cols, cz = args[1].shape[1:]
    width = args[2].shape[1] // 2
    heads = args[6].shape[1]
    feat = args[4].shape[1] // heads
    dims = (rows, toks, cols, ch, cz, width, heads, feat)
    flat = (args[0].reshape(rows * toks, ch), args[1].reshape(toks * cols, cz)) + args[2:6]
    flat += (args[6].T, args[7].T, args[8], args[9].T) + args[10:]
    pairs = toks * cols
    packed = rows * toks // 2
    dma = pltpu.SemaphoreType.DMA
    v = lambda *shape: pltpu.VMEM(shape, F32)
    outs = pl.pallas_call(
        functools.partial(kernel, nt, nj, dims),
        out_shape=(
            jax.ShapeDtypeStruct((rows * toks, ch), F32),
            jax.ShapeDtypeStruct((pairs, cz), F32),
        ),
        in_specs=[pl.BlockSpec(memory_space=pl.ANY)] * 12,
        out_specs=(pl.BlockSpec(memory_space=pl.ANY),) * 2,
        scratch_shapes=[v(*a.shape) for a in flat]
        + [
            v(rows * 8, LANES), v(toks // cols, rows * 4, LANES), v(packed, LANES), v(toks, LANES),
            v(nj, rows * 8, LANES), v(nj, rows * 4, LANES), v(nt, packed, LANES), v(nj, toks, LANES),
            v(pairs, width * width), v(pairs, cz), v(pairs, cz), v(pairs, cz), v(rows * toks, ch),
            dma((12,)), dma((2,)), dma((nj,)), dma((nt * toks // cols,)), dma((nt,)), dma((nj,)),
            dma((nj,)), dma((nj,)), dma((nt,)), dma((nj,)),
        ],
        compiler_params=pltpu.CompilerParams(
            collective_id=0, has_side_effects=True
        ),
    )(*flat)
    return outs[0].reshape(args[0].shape), outs[1].reshape(args[1].shape)


def solution(mesh):
    in_specs = (P("tj", "ti", None), P("ti", "tj", None)) + (P(),) * 10
    out_specs = (P("tj", "ti", None), P("ti", "tj", None))
    return jax.shard_map(
        functools.partial(shards, mesh.shape["ti"], mesh.shape["tj"]),
        mesh=mesh, in_specs=in_specs, out_specs=out_specs, check_vma=False,
    )
```
